256 devices in a mesh: dp: 64 (over z, y, core), mp: 4 (over x).
Axes of the slice: x: 4, y: 4, z: 8, core: 2. Of those that a mesh axis runs over, the one named last changes fastest.
Arguments:
- sample_inputs: bfloat16 [512, 512], P(('dp', 'mp')), may hold values from -6 to 6
- sample_outputs: bfloat16 [512, 1024], P(('dp', 'mp')), may hold values from -6 to 6
- directions: bfloat16 [512, 256, 512], P(('dp', 'mp')), may hold values from -24 to 24
- jacobian_targets: bfloat16 [512, 256, 1024], P(('dp', 'mp')), may hold values from -24 to 24
- jacobian_ranks: int32 [512], P(('dp', 'mp')), may hold values from 16 to 256, as said below
- encoder_weight: bfloat16 [512, 2048], replicated, may hold values from -0.25 to 0.25
- decoder_weight: bfloat16 [1024, 2048], replicated, may hold values from -0.125 to 0.125
Outputs:
- grad_encoder: float32 [512, 2048], P('dp', 'mp')
- grad_decoder: float32 [1024, 2048], P('dp', 'mp')
The draws below stay inside these ranges and needn't reach their ends.
Inputs may be any that keep to these rules, and one draw needn't show every extreme that they name: `jacobian_ranks`: every rank is a multiple of 16.
All inputs are finite; a program needn't handle non-finite values.
Results may differ from the reference program's by a relative error of at most 0.0013.
Values may be sent and summed in bfloat16 or wider, within the bound.
No kernel may reach another device: no remote copies, remote signals or barrier semaphores. Data moves between devices by JAX's collectives and lax.ppermute only.
A program may use at most 128 MiB of HBM per device.

```python
import math
import jax
import jax.numpy as jnp
from jax import lax

IN = 512
HID = 2048
OUT = 1024
RMAX = 256
BLK = 16
SAMP_DEV = 2
BMAX = 16
SAMPLES = 512


def draw_jacobian_ranks(key, part):
    devices_all = SAMPLES // SAMP_DEV
    light_low = max(1, BMAX // 16)
    light_high = max(light_low, BMAX * 8 // 16)
    heavy_low = max(1, BMAX * 5 // 16)
    heavy_high = max(heavy_low, BMAX * 9 // 16)
    heavy_device = jax.random.randint(jax.random.fold_in(key, 11), (), 0, devices_all)
    light_counts = jax.random.randint(jax.random.fold_in(key, 12), (devices_all, SAMP_DEV), light_low, light_high + 1)
    heavy_counts = jax.random.randint(jax.random.fold_in(key, 13), (SAMP_DEV,), heavy_low, heavy_high + 1)
    heavy_counts = heavy_counts.at[0].set(BMAX)
    device_ids = jnp.arange(devices_all)[:, None]
    block_counts = jnp.where(device_ids == heavy_device, heavy_counts[None, :], light_counts)
    return (block_counts.reshape(-1) * BLK).astype(jnp.int32)


def spiked(drawn, key, source, target, blocks, factor):
    owner, partner = [(jnp.arange(drawn.shape[position]) // (drawn.shape[position] // blocks)).reshape([-1 if axis == position else 1 for axis in range(drawn.ndim)]) for position in (source, target)]
    chosen = jax.random.permutation(key, blocks)[partner]
    strong = (owner == chosen) | (owner == (partner + blocks // 2) % blocks)
    return jnp.where(strong, factor * drawn, drawn)


def shard_levels(key, extent, cuts, least, top_value):
    factor_of = 1.0
    for dim, parts in cuts:
        heights = jax.random.uniform(jax.random.fold_in(jax.random.fold_in(key, 6), dim), (parts,), jnp.float32, least / len(cuts), top_value / len(cuts))
        factor_of = factor_of * jnp.repeat(jnp.exp(heights), extent[dim] // parts).reshape((-1,) + (1,) * (len(extent) - 1 - dim))
    return factor_of


def bell_draw(stream_key, extent, spread, reach, shards=(), kind=jnp.bfloat16):
    values = spread * jax.random.normal(stream_key, extent, jnp.float32)
    if shards:
        values = values * shard_levels(stream_key, extent, shards, -0.22, 0.18)
    return jnp.clip(values, -reach, reach).astype(kind)


def heavy_noise(own_key, extent, deviation, most, shards, heavy, kind=jnp.bfloat16):
    result = deviation * jax.random.normal(own_key, extent, jnp.float32)
    if shards:
        result = result * shard_levels(own_key, extent, shards, -0.22, 0.18)
    return jnp.clip(spiked(result, jax.random.fold_in(own_key, 3), *heavy), -most, most).astype(kind)


def setup_inputs(seed: int = 0) -> dict:
    key_of = jax.random.split(jax.random.key(seed), 8)
    return {
        "sample_inputs": bell_draw(key_of[0], (SAMPLES, IN), 1.0, 6.0, ((0, 256),)),
        "sample_outputs": bell_draw(key_of[1], (SAMPLES, OUT), 1.0, 6.0, ((0, 256),)),
        "directions": heavy_noise(key_of[2], (SAMPLES, RMAX, IN), 1.0, 24.0, ((0, 256),), (0, 2, 256, 6.0)),
        "jacobian_targets": heavy_noise(key_of[3], (SAMPLES, RMAX, OUT), 1.0, 24.0, ((0, 256),), (0, 2, 256, 6.0)),
        "jacobian_ranks": draw_jacobian_ranks(jax.random.fold_in(key_of[7], 71), 0),
        "encoder_weight": bell_draw(key_of[5], (IN, HID), IN ** -0.5, 0.25),
        "decoder_weight": bell_draw(key_of[6], (OUT, HID), HID ** -0.5, 0.125),
    }


contract_last = (((1,), (1,)), ((), ()))
contract_first = (((0,), (0,)), ((), ()))
tile_blocks = 64

def misfit_terms(sample_inputs, sample_outputs, encoder_weight, decoder_weight, factor):
    pre_act = jnp.dot(sample_inputs, encoder_weight, preferred_element_type=jnp.float32)
    hidden_act = jnp.tanh(pre_act)
    slopes = 1.0 - hidden_act * hidden_act
    act_rounded = hidden_act.astype(jnp.bfloat16)
    fitted = lax.dot_general(act_rounded, decoder_weight, contract_last, preferred_element_type=jnp.float32)
    misfit = fitted - sample_outputs.astype(jnp.float32)
    misfit_grad = (factor * misfit).astype(jnp.bfloat16)
    grad_decoder = lax.dot_general(misfit_grad, act_rounded, contract_first, preferred_element_type=jnp.float32)
    back_misfit = jnp.dot(misfit_grad, decoder_weight, preferred_element_type=jnp.float32)
    entered = (back_misfit * slopes).astype(jnp.bfloat16)
    grad_encoder = lax.dot_general(sample_inputs, entered, contract_first, preferred_element_type=jnp.float32)
    return (grad_encoder, grad_decoder)

def block_terms(block_dirs, block_targets, row_values, weights, encoder_weight, decoder_weight, totals):
    grad_encoder, grad_decoder = totals
    count_blocks = block_dirs.shape[0]
    block_cols = block_dirs.shape[1]
    in_width = block_dirs.shape[2]
    out_width = block_targets.shape[2]
    hidden = encoder_weight.shape[1]
    pre_act = jnp.dot(row_values, encoder_weight, preferred_element_type=jnp.float32)
    hidden_act = jnp.tanh(pre_act)
    slopes = 1.0 - hidden_act * hidden_act
    columns = block_dirs.reshape(count_blocks * block_cols, in_width)
    along_hidden = jnp.dot(columns, encoder_weight, preferred_element_type=jnp.float32)
    along_hidden = along_hidden.reshape(count_blocks, block_cols, hidden)
    pushed = (along_hidden * slopes[:, None, :]).astype(jnp.bfloat16).reshape(count_blocks * block_cols, hidden)
    images = lax.dot_general(pushed, decoder_weight, contract_last, preferred_element_type=jnp.float32)
    misfit_cols = images.reshape(count_blocks, block_cols, out_width) - block_targets.astype(jnp.float32)
    jac_grad = (misfit_cols * weights[:, None, None]).astype(jnp.bfloat16).reshape(count_blocks * block_cols, out_width)
    grad_decoder = grad_decoder + lax.dot_general(jac_grad, pushed, contract_first, preferred_element_type=jnp.float32)
    backward = jnp.dot(jac_grad, decoder_weight, preferred_element_type=jnp.float32).reshape(count_blocks, block_cols, hidden)
    lifted = (backward * slopes[:, None, :]).astype(jnp.bfloat16).reshape(count_blocks * block_cols, hidden)
    curvature = -2.0 * hidden_act[:, None, :] * slopes[:, None, :] * backward * along_hidden
    sum_curve = lax.optimization_barrier(jnp.sum(curvature, axis=1))
    grad_encoder = grad_encoder + lax.dot_general(columns, lifted, contract_first, preferred_element_type=jnp.float32)
    grad_encoder = grad_encoder + lax.dot_general(row_values.astype(jnp.float32), sum_curve, contract_first, precision=lax.Precision.HIGHEST)
    return (grad_encoder, grad_decoder)

def reference(sample_inputs, sample_outputs, directions, jacobian_targets, jacobian_ranks, encoder_weight, decoder_weight):
    factor = 2.0 / math.sqrt(SAMPLES)
    totals = misfit_terms(sample_inputs, sample_outputs, encoder_weight, decoder_weight, factor)
    slot_total = SAMPLES * BMAX
    flat_dirs = directions.reshape(slot_total, BLK, IN)
    flat_targets = jacobian_targets.reshape(slot_total, BLK, OUT)
    counts = (jacobian_ranks // BLK).astype(jnp.int32)
    positions = jnp.arange(slot_total, dtype=jnp.int32)
    owners_all = (positions // BMAX).astype(jnp.int32)
    active = positions % BMAX < counts[owners_all]
    ordering = jnp.argsort(jnp.where(active, positions, positions + slot_total)).astype(jnp.int32)
    held_count = jnp.sum(active.astype(jnp.int32))
    padded_order = jnp.concatenate([ordering, jnp.zeros((tile_blocks,), jnp.int32)])
    slot_weight = factor * (BLK / jacobian_ranks.astype(jnp.float32))

    def tile_step(step_index, state):
        first_slot = (step_index * tile_blocks).astype(jnp.int32)
        chosen = lax.dynamic_slice(padded_order, (first_slot,), (tile_blocks,))
        in_use = first_slot + jnp.arange(tile_blocks, dtype=jnp.int32) < held_count
        owners = (chosen // BMAX).astype(jnp.int32)
        weights = jnp.where(in_use, slot_weight[owners], 0.0)
        row_values = jnp.take(sample_inputs, owners, axis=0)
        return block_terms(jnp.take(flat_dirs, chosen, axis=0), jnp.take(flat_targets, chosen, axis=0), row_values, weights, encoder_weight, decoder_weight, state)
    trips = (held_count + tile_blocks - 1) // tile_blocks
    grad_encoder, grad_decoder = lax.fori_loop(0, trips, tile_step, totals)
    return (grad_encoder, grad_decoder)
```

```python
import functools
import math

import jax
import jax.numpy as jnp
from jax import lax
from jax.experimental import pallas as pl
from jax.experimental.pallas import tpu as pltpu
from jax.sharding import PartitionSpec as P

F32 = jnp.float32
BF16 = jnp.bfloat16
S16 = jnp.int16
BLK = 16
EXTRA = 16
KT = 256
COLS = 512
DEC = 16
ENC = 8
TOP = 32700.0
TINY = 1e-30
MIB = 1 << 20

NN = (((1,), (0,)), ((), ()))
NT = (((1,), (1,)), ((), ()))


def dot(a, b, dims=NN):
    return lax.dot_general(a, b, dims, preferred_element_type=F32)


def message_rows(blocks):
    return 16 + DEC * blocks + max(16, ENC * blocks)


def exponents(largest):
    return jnp.floor(jnp.log(jnp.maximum(largest, TINY)) * (1.0 / math.log(2.0))) + 1.0


def power(e):
    return jnp.exp(e * math.log(2.0))


def twice(v, rows):
    return jnp.concatenate([v] * (rows // 8), axis=0) if rows > 8 else v


def coded(x, mult):
    return jnp.round(x * twice(mult, x.shape[0])).astype(jnp.int32).astype(S16)


def fold_max(best, x):
    for r in range(0, x.shape[0], 8):
        best = jnp.maximum(best, jnp.abs(x[r : r + 8]))
    return best


def write_scales(msg, best_dec, best_enc):
    e_dec, e_enc = exponents(best_dec), exponents(best_enc)
    both = jnp.concatenate([e_dec, e_enc], axis=0)
    msg[0:16, :] = both.astype(jnp.int32).astype(S16)
    return power(-e_dec) * TOP, power(-e_enc) * TOP


def read_scales(msg):
    both = msg[0:16, :].astype(jnp.int32).astype(F32)
    s = power(both) * (1.0 / TOP)
    return s[0:8], s[8:16]


def plain(q, mult):
    return q.astype(jnp.int32).astype(F32) * twice(mult, q.shape[0])


def rows_loop(count, step, body, init):
    n = count // step
    if n == 1:
        return body(0, init)
    unroll = 4 if n % 4 == 0 else (2 if n % 2 == 0 else 1)

    def it(i, carry):
        for u in range(unroll):
            carry = body(pl.multiple_of((i * unroll + u) * step, step), carry)
        return carry

    return lax.fori_loop(0, n // unroll, it, init)


def encode_rows(src, src_start, count, msg, msg_start, mult):
    step = min(16, count)

    def body(o, carry):
        x = src[pl.ds(src_start + o, step), :]
        msg[pl.ds(msg_start + o, step), :] = coded(x, mult)
        return carry

    rows_loop(count, step, body, 0)


def step_kernel(spec, n_msgs, sizes, *refs):
    groups, keep_blocks, out_sizes = spec
    state_dec, state_enc = refs[0], refs[1]
    msgs = refs[2 : 2 + n_msgs]
    outs = refs[2 + n_msgs :]
    new_dec, new_enc = outs[0], outs[1]
    sent = outs[2 : 2 + len(out_sizes)]
    hold_dec, hold_enc = outs[2 + len(out_sizes) :] if out_sizes else (None, None)
    scales = [read_scales(m) for m in msgs]
    zero = jnp.zeros((8, COLS), F32)
    best = [[zero, zero] for _ in out_sizes]
    pending = []
    held = 0
    for start, blocks, arrived, dest in groups:
        for part, per, state, new, hold in (
            (0, DEC, state_dec, new_dec, hold_dec),
            (1, ENC, state_enc, new_enc, hold_enc),
        ):
            count = per * blocks
            step = min(16, count)

            def value(o, part=part, per=per, state=state, start=start, arrived=arrived, step=step):
                x = state[pl.ds(start * per + o, step), :]
                for m, at in arrived:
                    base = 16 + (DEC * sizes[m] if part else 0) + per * at
                    x = x + plain(msgs[m][pl.ds(base + o, step), :], scales[m][part])
                return x

            if dest[0] == "keep":
                at = dest[1] * per

                def body(o, carry, value=value, new=new, at=at, step=step):
                    new[pl.ds(at + o, step), :] = value(o)
                    return carry

                rows_loop(count, step, body, 0)
            else:
                at = held * per

                def body(o, carry, value=value, hold=hold, at=at, step=step):
                    x = value(o)
                    hold[pl.ds(at + o, step), :] = x
                    return fold_max(carry, x)

                best[dest[1]][part] = rows_loop(count, step, body, best[dest[1]][part])
        if dest[0] == "send":
            pending.append((held, blocks, dest[1], dest[2]))
            held += blocks
    mults = [write_scales(sent[j], *best[j]) for j in range(len(out_sizes))]
    for at, blocks, j, to in pending:
        encode_rows(hold_dec, at * DEC, blocks * DEC, sent[j], 16 + to * DEC, mults[j][0])
        base = 16 + out_sizes[j] * DEC + to * ENC
        if blocks == 1:
            x = coded(hold_enc[at * ENC : at * ENC + 8, :], mults[j][1])
            sent[j][base : base + 8, :] = x
            sent[j][base + 8 : base + 16, :] = jnp.zeros((8, COLS), S16)
        else:
            encode_rows(hold_enc, at * ENC, blocks * ENC, sent[j], base, mults[j][1])


def reduce_step(name, groups, keep_blocks, in_sizes, out_sizes, state, msgs):
    held = sum(g[1] for g in groups if g[3][0] == "send")
    out_shape = [
        jax.ShapeDtypeStruct((keep_blocks * DEC, COLS), F32),
        jax.ShapeDtypeStruct((keep_blocks * ENC, COLS), F32),
    ] + [jax.ShapeDtypeStruct((message_rows(n), COLS), S16) for n in out_sizes]
    scratch = []
    if out_sizes:
        scratch = [pltpu.VMEM((held * DEC, COLS), F32), pltpu.VMEM((held * ENC, COLS), F32)]
    vmem = pl.BlockSpec(memory_space=pltpu.VMEM)
    outs = pl.pallas_call(
        functools.partial(step_kernel, (groups, keep_blocks, out_sizes), len(msgs), in_sizes),
        out_shape=out_shape,
        in_specs=[vmem] * (2 + len(msgs)),
        out_specs=[vmem] * len(out_shape),
        scratch_shapes=scratch,
        compiler_params=pltpu.CompilerParams(vmem_limit_bytes=40 * MIB),
        name=name,
    )(*state, *msgs)
    return outs[:2], outs[2:]


def step_specs():
    core = []
    for h in (0, 1):
        core.append((h * 64, 32, ((0, h * 64),), ("keep", h * 32)))
        core.append((h * 64 + 32, 32, ((0, h * 64 + 32),), ("send", h, 0)))
    a1 = []
    for h in (0, 1):
        a1.append((h * 32, 16, ((h, 0),), ("keep", h * 16)))
        a1.append((h * 32 + 16, 16, ((h, 16),), ("send", h, 0)))
    a2 = []
    for h in (0, 1):
        for b in range(4):
            dest = ("keep", h * 4) if b == 0 else ("send", b - 1, h * 4)
            a2.append((h * 16 + b * 4, 4, ((h, b * 4),), dest))
    b = [
        (0, 4, tuple((k, 0) for k in range(3)), ("keep", 0)),
        (4, 4, tuple((k, 4) for k in range(3)), ("send", 0, 0)),
    ]
    z1 = [(0, 1, ((0, 0),), ("keep", 0))]
    z1 += [(i, 1, ((0, i),), ("send", i - 1, 0)) for i in (1, 2, 3)]
    z2 = [(0, 1, tuple((k, 0) for k in range(3)), ("keep", 0))]
    return (
        ("core", core, 64, (128,), (32, 32)),
        ("a1", a1, 32, (32, 32), (16, 16)),
        ("a2", a2, 8, (16, 16), (8, 8, 8)),
        ("b", b, 4, (8, 8, 8), (4,)),
        ("z1", z1, 1, (4,), (1, 1, 1)),
        ("z2", z2, 1, (1, 1, 1), ()),
    )


def terms_kernel(
    factor,
    ranks,
    table,
    x_ref,
    y_ref,
    dirs,
    targets,
    enc,
    dec,
    mine_dec,
    mine_enc,
    msg,
    along_s,
    pushed,
    lifted,
    jac,
    cols,
    jac_t,
    cols_t,
    out_dec,
    out_enc,
):
    hidden = enc.shape[1]
    in_width = enc.shape[0]
    out_width = dec.shape[0]
    rmax = dirs.shape[1]
    r0, r1 = ranks[0], ranks[1]
    ends = (EXTRA, pl.multiple_of(EXTRA + r0, BLK))
    tail = pl.multiple_of(EXTRA + rmax + r0, BLK)
    for ref in (pushed, lifted, jac, cols):
        ref[pl.ds(tail, KT), :] = jnp.zeros((KT, ref.shape[1]), BF16)

    def pair(ref):
        v = ref[...].astype(F32)
        odd = lax.broadcasted_iota(jnp.int32, (EXTRA, v.shape[1]), 0) % 2 == 1
        top = jnp.broadcast_to(v[0:1], odd.shape)
        return jnp.where(odd, jnp.broadcast_to(v[1:2], odd.shape), top)

    x16 = pair(x_ref).astype(BF16)
    y16 = pair(y_ref)
    cols[0:EXTRA, :] = x16
    hid = jnp.tanh(dot(x16, enc[...]))
    slopes = 1.0 - hid * hid
    act = hid.astype(BF16)
    pushed[0:EXTRA, :] = act
    row = lax.broadcasted_iota(jnp.int32, (EXTRA, out_width), 0)
    misfit_grad = (factor * (dot(act, dec[...], NT) - y16)).astype(BF16)
    jac[0:EXTRA, :] = jnp.where(row < 2, misfit_grad.astype(F32), 0.0).astype(BF16)
    entered = dot(misfit_grad, dec[...]) * slopes

    sums = []
    for s in (0, 1):
        at = ends[s]
        rank = ranks[s]
        d = dirs[s]
        cols[pl.ds(at, rmax), :] = d
        for n in range(0, hidden, COLS):
            al = dot(d, enc[:, n : n + COLS])
            along_s[:, n : n + COLS] = al
            pushed[pl.ds(at, rmax), n : n + COLS] = (al * slopes[s : s + 1, n : n + COLS]).astype(BF16)
        weight = (factor * BLK) / jnp.full((rmax, COLS), rank, jnp.int32).astype(F32)
        live = lax.broadcasted_iota(jnp.int32, (rmax, COLS), 0) < rank
        weight = jnp.where(live, weight, 0.0)
        p = pushed[pl.ds(at, rmax), :]
        for n in range(0, out_width, COLS):
            im = dot(p, dec[n : n + COLS, :], NT)
            diff = im - targets[s, :, n : n + COLS].astype(F32)
            jac[pl.ds(at, rmax), n : n + COLS] = (diff * weight).astype(BF16)
        j = jac[pl.ds(at, rmax), :]
        curve = []
        for n in range(0, hidden, COLS):
            back = dot(j, dec[:, n : n + COLS])
            sl = slopes[s : s + 1, n : n + COLS]
            lifted[pl.ds(at, rmax), n : n + COLS] = (back * sl).astype(BF16)
            total = jnp.sum(back * along_s[:, n : n + COLS], axis=0, keepdims=True)
            curve.append(-2.0 * hid[s : s + 1, n : n + COLS] * sl * total)
        sums.append(jnp.concatenate(curve, axis=1))
    row = lax.broadcasted_iota(jnp.int32, (EXTRA, hidden), 0)
    sc = jnp.where(row % 2 == 1, jnp.broadcast_to(sums[1], row.shape), jnp.broadcast_to(sums[0], row.shape))
    hi = sc.astype(BF16).astype(F32)
    mid = (sc - hi).astype(BF16).astype(F32)
    low = sc - hi - mid
    ent = entered.astype(BF16).astype(F32)
    rest = jnp.where(row < 6, mid, jnp.where(row < 8, low, 0.0))
    lifted[0:EXTRA, :] = jnp.where(row < 2, ent, jnp.where(row < 4, hi, rest)).astype(BF16)

    passes = (EXTRA + r0 + r1 + KT - 1) // KT
    for many in (1, 2, 3):

        @pl.when(passes == many)
        def _(many=many):
            depth = KT * many
            for k in range(0, depth, KT):
                for n in range(0, out_width, KT):
                    jac_t[n : n + KT, k : k + KT] = jac[k : k + KT, n : n + KT].T
                for n in range(0, in_width, KT):
                    cols_t[n : n + KT, k : k + KT] = cols[k : k + KT, n : n + KT].T

            def column_block(xb, carry):
                at = pl.ds(pl.multiple_of(xb * COLS, COLS), COLS)
                pb = pushed[0:depth, at]
                for n in range(0, out_width, KT):
                    g = dot(jac_t[n : n + KT, 0:depth], pb)
                    for r in range(0, KT, DEC):
                        to = table[xb * 64 + (n + r) // DEC]
                        out_dec[pl.ds(pl.multiple_of(to * DEC, DEC), DEC), :] = g[r : r + DEC]
                lb = lifted[0:depth, at]
                for n in range(0, in_width, KT):
                    g = dot(cols_t[n : n + KT, 0:depth], lb)
                    for r in range(0, KT, ENC):
                        to = table[xb * 64 + (n + r) // ENC]
                        out_enc[pl.ds(pl.multiple_of(to * ENC, ENC), ENC), :] = g[r : r + ENC]
                return carry

            lax.fori_loop(0, hidden // COLS, column_block, 0)

    blocks = mine_dec.shape[0] // DEC
    half_dec, half_enc = blocks * DEC, blocks * ENC

    def copy_and_max(src, dst, half):
        def body(o, best):
            dst[pl.ds(o, 16), :] = src[pl.ds(o, 16), :]
            return fold_max(best, src[pl.ds(half + o, 16), :])

        return rows_loop(half, 16, body, jnp.zeros((8, COLS), F32))

    best_dec = copy_and_max(out_dec, mine_dec, half_dec)
    best_enc = copy_and_max(out_enc, mine_enc, half_enc)
    m_dec, m_enc = write_scales(msg, best_dec, best_enc)
    encode_rows(out_dec, half_dec, half_dec, msg, 16, m_dec)
    encode_rows(out_enc, half_enc, half_enc, msg, 16 + half_dec, m_enc)


def own_terms(factor, ranks, table, x, y, dirs, targets, enc, dec):
    rmax = dirs.shape[1]
    in_width, hidden = enc.shape
    out_width = dec.shape[0]
    rows = EXTRA + 2 * rmax + KT
    depth = -(-(EXTRA + 2 * rmax) // KT) * KT
    blocks = (out_width // DEC) * (hidden // COLS) // 2
    vmem = pl.BlockSpec(memory_space=pltpu.VMEM)
    smem = pl.BlockSpec(memory_space=pltpu.SMEM)
    outs = pl.pallas_call(
        functools.partial(terms_kernel, factor),
        out_shape=[
            jax.ShapeDtypeStruct((blocks * DEC, COLS), F32),
            jax.ShapeDtypeStruct((blocks * ENC, COLS), F32),
            jax.ShapeDtypeStruct((message_rows(blocks), COLS), S16),
        ],
        in_specs=[smem, smem] + [vmem] * 6,
        out_specs=[vmem] * 3,
        scratch_shapes=[
            pltpu.VMEM((rmax, hidden), F32),
            pltpu.VMEM((rows, hidden), BF16),
            pltpu.VMEM((rows, hidden), BF16),
            pltpu.VMEM((rows, out_width), BF16),
            pltpu.VMEM((rows, in_width), BF16),
            pltpu.VMEM((out_width, depth), BF16),
            pltpu.VMEM((in_width, depth), BF16),
            pltpu.VMEM((2 * blocks * DEC, COLS), F32),
            pltpu.VMEM((2 * blocks * ENC, COLS), F32),
        ],
        compiler_params=pltpu.CompilerParams(vmem_limit_bytes=60 * MIB),
        name="terms",
    )(ranks, table, x, y, dirs, targets, enc, dec)
    return outs[:2], outs[2:]


def place_table(z, y, core, x):
    i = jnp.arange(256, dtype=jnp.int32)
    xb, zb, yb, cb = i // 64, (i // 8) % 8, (i // 2) % 4, i % 2
    odd = (zb ^ z) & 1
    zi = ((zb - (z ^ odd)) & 7) >> 1
    first = cb == 0
    ea = jnp.where(first, xb ^ x, yb ^ y)
    eb = jnp.where(first, yb - y, xb - x) & 3
    ap = jnp.where(ea == 0, 0, jnp.where(ea == 2, 3, jnp.where((ea == 3) == (odd == 0), 1, 2)))
    group = jnp.where(cb == core, 0, 128)
    return group + odd * 64 + ap * 16 + eb * 4 + zi


def partners(fn):
    pairs = []
    for z in range(8):
        for y in range(4):
            for c in range(2):
                for x in range(4):
                    z2, y2, c2, x2 = fn(z, y, c, x)
                    pairs.append((((z * 4 + y) * 2 + c) * 4 + x, ((z2 * 4 + y2) * 2 + c2) * 4 + x2))
    return pairs


def send(value, fn):
    return lax.ppermute(value, ("dp", "mp"), partners(fn))


def first_axis(flip):
    return lambda z, y, c, x: (z, y, c, x ^ flip) if c == 0 else (z, y ^ flip, c, x)


def second_axis(k):
    return lambda z, y, c, x: (z, (y + k) % 4, c, x) if c == 0 else (z, y, c, (x + k) % 4)


def z_axis(k):
    return lambda z, y, c, x: ((z + k) % 8, y, c, x)


def per_device(sample_inputs, sample_outputs, directions, targets, ranks, enc, dec):
    population = sample_inputs.shape[0] * lax.axis_size("dp") * lax.axis_size("mp")
    factor = 2.0 / math.sqrt(population)
    dp = lax.axis_index("dp")
    x = lax.axis_index("mp")
    z, y, core = dp // 8, (dp // 2) % 4, dp % 2
    table = place_table(z, y, core, x)
    state, msgs = own_terms(
        factor, ranks, table, sample_inputs, sample_outputs, directions, targets, enc, dec
    )
    routes = (
        [lambda z, y, c, x: (z, y, 1 - c, x)],
        [first_axis(1), first_axis(3)],
        [first_axis(3), first_axis(1)],
        [second_axis(k) for k in (1, 2, 3)],
        [lambda z, y, c, x: (z ^ 1, y, c, x)],
        [z_axis(2 * k) for k in (1, 2, 3)],
    )
    for route, (name, groups, keep, in_sizes, out_sizes) in zip(routes, step_specs()):
        arrived = [send(m, fn) for m, fn in zip(msgs, route)]
        state, msgs = reduce_step(name, groups, keep, in_sizes, out_sizes, state, arrived)
    return state[1], state[0]


def solution(mesh):
    both = ("dp", "mp")
    in_specs = (
        P(both, None),
        P(both, None),
        P(both, None, None),
        P(both, None, None),
        P(both),
        P(),
        P(),
    )
    return jax.shard_map(
        per_device,
        mesh=mesh,
        in_specs=in_specs,
        out_specs=(P("dp", "mp"), P("dp", "mp")),
        check_vma=False,
    )
```

```python
import functools
import math

import jax
import jax.numpy as jnp
from jax import lax
from jax.experimental import pallas as pl
from jax.experimental.pallas import tpu as pltpu
from jax.sharding import PartitionSpec as P

F32 = jnp.float32
BF16 = jnp.bfloat16
S16 = jnp.int16
BLK = 16
EXTRA = 16
COLS = 512
PER = (16, 8)
TOP = 32700.0
TINY = 1e-30
MIB = 1 << 20
SIZES = ((256, 256), (416, 512), (528, 640))
ROWS = 784

NN = (((1,), (0,)), ((), ()))
NT = (((1,), (1,)), ((), ()))
VM = pl.BlockSpec(memory_space=pltpu.VMEM)
SM = pl.BlockSpec(memory_space=pltpu.SMEM)
HB = pl.BlockSpec(memory_space=pltpu.HBM)


def dot(a, b, dims=NN):
    return lax.dot_general(a, b, dims, preferred_element_type=F32)


def section_base(sections, index):
    return 16 + sum(PER[p] * n for p, n in sections[:index])


def message_rows(sections):
    rows = section_base(sections, len(sections))
    return -(-rows // 16) * 16


def exponents(largest):
    return jnp.floor(jnp.log(jnp.maximum(largest, TINY)) * (1.0 / math.log(2.0))) + 1.0


def power(e):
    return jnp.exp(e * math.log(2.0))


def twice(v, rows):
    return jnp.concatenate([v] * (rows // 8), axis=0) if rows > 8 else v


def coded(x, mult):
    return jnp.round(x * twice(mult, x.shape[0])).astype(jnp.int32).astype(S16)


def plain(q, mult):
    return q.astype(jnp.int32).astype(F32) * twice(mult, q.shape[0])


def fold_max(best, x):
    for r in range(0, x.shape[0], 8):
        best = jnp.maximum(best, jnp.abs(x[r : r + 8]))
    return best


def write_scales(msg, best):
    es = [exponents(b) for b in best]
    msg[0:16, :] = jnp.concatenate([es[0], es[-1]], axis=0).astype(jnp.int32).astype(S16)
    return [power(-e) * TOP for e in es]


def read_scales(msg):
    s = power(msg[0:16, :].astype(jnp.int32).astype(F32)) * (1.0 / TOP)
    return s[0:8], s[8:16]


def rows_loop(count, step, body, init):
    n = count // step
    if n == 1:
        return body(0, init)
    unroll = 4 if n % 4 == 0 else (2 if n % 2 == 0 else 1)

    def it(i, carry):
        for u in range(unroll):
            carry = body(pl.multiple_of((i * unroll + u) * step, step), carry)
        return carry

    return lax.fori_loop(0, n // unroll, it, init)


def encode_rows(src, src_start, count, msg, msg_start, mult):
    def body(o, carry):
        msg[pl.ds(msg_start + o, 16), :] = coded(src[pl.ds(src_start + o, 16), :], mult)
        return carry

    rows_loop(count, 16, body, 0)


def step_kernel(parts, groups, ins, outs, *refs):
    np_ = len(parts)
    states = dict(zip(parts, refs[:np_]))
    msgs = refs[np_ : np_ + len(ins)]
    rest = refs[np_ + len(ins) :]
    news = dict(zip(parts, rest[:np_]))
    sent = rest[np_ : np_ + len(outs)]
    holds = dict(zip(parts, rest[np_ + len(outs) :]))
    scales = [read_scales(m) for m in msgs]
    zero = jnp.zeros((8, COLS), F32)
    best = [[zero] * len(o) for o in outs]
    pending = []
    held = {p: 0 for p in parts}
    for part, start, blocks, arrived, dest in groups:
        per = PER[part]
        count = per * blocks
        step = min(16, count)

        def value(o, part=part, per=per, start=start, arrived=arrived, step=step):
            x = states[part][pl.ds(start * per + o, step), :]
            for m, at in arrived:
                index = [p for p, _ in ins[m]].index(part)
                base = section_base(ins[m], index) + per * at
                x = x + plain(msgs[m][pl.ds(base + o, step), :], scales[m][index])
            return x

        if dest[0] == "keep":
            to = dest[1] * per

            def body(o, carry, value=value, part=part, to=to, step=step):
                news[part][pl.ds(to + o, step), :] = value(o)
                return carry

            rows_loop(count, step, body, 0)
        else:
            index = [p for p, _ in outs[dest[1]]].index(part)
            to = held[part] * per

            def body(o, carry, value=value, part=part, to=to, step=step):
                x = value(o)
                holds[part][pl.ds(to + o, step), :] = x
                return fold_max(carry, x)

            best[dest[1]][index] = rows_loop(count, step, body, best[dest[1]][index])
            pending.append((part, to, count, dest[1], index, dest[2] * per))
            held[part] += blocks
    mults = [write_scales(sent[j], best[j]) for j in range(len(outs))]
    for part, at, count, j, index, to in pending:
        base = section_base(outs[j], index) + to
        if count < 16:
            x = coded(holds[part][at : at + 8, :], mults[j][index])
            sent[j][base : base + 8, :] = x
            sent[j][base + 8 : base + 16, :] = jnp.zeros((8, COLS), S16)
        else:
            encode_rows(holds[part], at, count, sent[j], base, mults[j][index])


def reduce_step(name, parts, groups, keep, ins, outs, states, msgs):
    scratch = []
    if outs:
        for p in parts:
            held = sum(g[2] for g in groups if g[0] == p and g[4][0] == "send")
            scratch.append(pltpu.VMEM((held * PER[p], COLS), F32))
    out_shape = [jax.ShapeDtypeStruct((keep * PER[p], COLS), F32) for p in parts]
    out_shape += [jax.ShapeDtypeStruct((message_rows(o), COLS), S16) for o in outs]
    got = pl.pallas_call(
        functools.partial(step_kernel, parts, groups, ins, outs),
        out_shape=out_shape,
        in_specs=[VM] * (len(parts) + len(msgs)),
        out_specs=[VM] * len(out_shape),
        scratch_shapes=scratch,
        compiler_params=pltpu.CompilerParams(vmem_limit_bytes=16 * MIB),
        cost_estimate=pl.CostEstimate(flops=int(2e8) * keep, transcendentals=0, bytes_accessed=0),
        name=name,
    )(*states, *msgs)
    return got[: len(parts)], got[len(parts) :]


def core_groups(part):
    groups = []
    for h in (0, 1):
        groups.append((part, h * 64, 32, ((0, h * 64),), ("keep", h * 32)))
        groups.append((part, h * 64 + 32, 32, ((0, h * 64 + 32),), ("send", h, 0)))
    return tuple(groups)


def first_groups(part):
    groups = []
    for h in (0, 1):
        groups.append((part, h * 32, 16, ((h, 0),), ("keep", h * 16)))
        groups.append((part, h * 32 + 16, 16, ((h, 16),), ("send", h, 0)))
    return tuple(groups)


def join_groups():
    groups = []
    for part in (0, 1):
        for h in (0, 1):
            for b in range(4):
                dest = ("keep", h * 4) if b == 0 else ("send", b - 1, h * 4)
                groups.append((part, h * 16 + b * 4, 4, ((part * 2 + h, b * 4),), dest))
    return tuple(groups)


def second_groups():
    groups = []
    for part in (0, 1):
        groups.append((part, 0, 4, tuple((k, 0) for k in range(3)), ("keep", 0)))
        groups.append((part, 4, 4, tuple((k, 4) for k in range(3)), ("send", 0, 0)))
    return tuple(groups)


def half_groups(n):
    groups = []
    for part in (0, 1):
        groups.append((part, 0, n, ((0, 0),), ("keep", 0)))
        groups.append((part, n, n, ((0, n),), ("send", 0, 0)))
    return tuple(groups)


def last_groups():
    return tuple((part, 0, 1, ((0, 0),), ("keep", 0)) for part in (0, 1))


def sections(n):
    return ((0, n), (1, n))


def by_size(total, body):
    low = 0
    for rows, depth in SIZES:

        @pl.when((total > low) & (total <= rows))
        def _(rows=rows, depth=depth):
            body(rows, depth)

        low = rows


def second_rows(rows, r0, width):
    row = lax.broadcasted_iota(jnp.int32, (rows, width), 0)
    return ((row < EXTRA) & (row % 2 == 1)) | (row >= EXTRA + r0)


def spread(second, v0, v1):
    return jnp.where(second, jnp.broadcast_to(v1, second.shape), jnp.broadcast_to(v0, second.shape))


def transposed(src, dst, width, depth):
    for k in range(0, depth, 128):
        for n in range(0, width, 512):
            dst[n : n + 512, k : k + 128] = src[k : k + 128, n : n + 512].T


def products(per, lhs_t, rhs, depth, width, hidden, table, both):
    def column_block(xb, carry):
        b = rhs[0:depth, pl.ds(pl.multiple_of(xb * COLS, COLS), COLS)]
        for n in range(0, width, 256):
            g = dot(lhs_t[n : n + 256, 0:depth], b)
            for r in range(0, 256, per):
                to = table[xb * 64 + (n + r) // per]
                both[pl.ds(pl.multiple_of(to * per, per), per), :] = g[r : r + per]
        return carry

    lax.fori_loop(0, hidden // COLS, column_block, 0)


def encode_other(both, msg):
    half = both.shape[0] // 2
    zero = jnp.zeros((8, COLS), F32)
    best = rows_loop(half, 16, lambda o, c: fold_max(c, both[pl.ds(half + o, 16), :]), zero)
    (mult,) = write_scales(msg, [best])
    encode_rows(both, half, half, msg, 16, mult)


def decoder_kernel(
    factor, ranks, table, x_ref, y_ref, dirs, targets, enc, dec,
    both, msg, jac, along, cols, hid, dec_v,
    enc_v, dirs_v, targets_v, tgt, pushed, jac_t, sems,
):
    in_width, hidden = enc.shape
    out_width = dec.shape[0]
    rmax = dirs.shape[1]
    copies = [
        pltpu.make_async_copy(a, b, sems.at[i])
        for i, (a, b) in enumerate(
            ((dirs, dirs_v), (enc, enc_v), (dec, dec_v), (targets, targets_v))
        )
    ]
    for c in copies:
        c.start()
    r0, r1 = ranks[0], ranks[1]
    at1 = pl.multiple_of(EXTRA + r0, BLK)
    tail = pl.multiple_of(EXTRA + rmax + r0, BLK)
    for ref in (cols, tgt):
        ref[pl.ds(tail, 256), :] = jnp.zeros((256, ref.shape[1]), BF16)

    def pair(ref):
        v = ref[...].astype(F32)
        odd = lax.broadcasted_iota(jnp.int32, (EXTRA, v.shape[1]), 0) % 2 == 1
        return spread(odd, v[0:1], v[1:2]).astype(BF16)

    cols[0:EXTRA, :] = pair(x_ref)
    tgt[0:EXTRA, :] = pair(y_ref)
    copies[0].wait()
    cols[EXTRA : EXTRA + rmax, :] = dirs_v[0]
    cols[pl.ds(at1, rmax), :] = dirs_v[1]
    copies[1].wait()

    def forward(rows, depth):
        second = second_rows(rows, r0, COLS)
        first_row = lax.broadcasted_iota(jnp.int32, (rows, COLS), 0)
        if depth > rows:
            for ref in (pushed, jac):
                ref[rows:depth, :] = jnp.zeros((depth - rows, ref.shape[1]), BF16)

        def hidden_block(n, carry):
            at = pl.ds(pl.multiple_of(n * COLS, COLS), COLS)
            al = dot(cols[0:rows, :], enc_v[:, at])
            along[0:rows, at] = al
            h = jnp.tanh(al[0:EXTRA])
            hid[:, at] = h
            s = 1.0 - h * h
            sl = spread(second, s[0:1], s[1:2])
            pushed[0:rows, at] = (al * sl).astype(BF16)
            pushed[0:EXTRA, at] = h.astype(BF16)
            return carry

        lax.fori_loop(0, hidden // COLS, hidden_block, 0)

        copies[2].wait()
        copies[3].wait()
        tgt[EXTRA : EXTRA + rmax, :] = targets_v[0]
        tgt[pl.ds(at1, rmax), :] = targets_v[1]

        def weight_of(rank):
            return (factor * BLK) / jnp.full((rows, COLS), rank, jnp.int32).astype(F32)

        w = jnp.where(first_row >= EXTRA + r0, weight_of(r1), weight_of(r0))
        w = jnp.where(first_row < EXTRA, jnp.where(first_row < 2, factor, 0.0), w)
        w = jnp.where(first_row < EXTRA + r0 + r1, w, 0.0)

        def output_block(n, carry):
            at = pl.ds(pl.multiple_of(n * COLS, COLS), COLS)
            im = dot(pushed[0:rows, :], dec_v[at, :], NT)
            jac[0:rows, at] = ((im - tgt[0:rows, at].astype(F32)) * w).astype(BF16)
            return carry

        lax.fori_loop(0, out_width // COLS, output_block, 0)
        transposed(jac, jac_t, out_width, depth)
        products(PER[0], jac_t, pushed, depth, out_width, hidden, table, both)

    by_size(EXTRA + r0 + r1, forward)
    encode_other(both, msg)


def encoder_kernel(
    ranks, table, jac, along, cols, hid, dec, both, msg, lifted, cols_t
):
    in_width = cols.shape[1]
    hidden = dec.shape[1]
    r0, r1 = ranks[0], ranks[1]

    def backward(rows, depth):
        second = second_rows(rows, r0, COLS)
        extra_row = lax.broadcasted_iota(jnp.int32, (EXTRA, COLS), 0)
        if depth > rows:
            lifted[rows:depth, :] = jnp.zeros((depth - rows, hidden), BF16)

        def hidden_block(n, carry):
            at = pl.ds(pl.multiple_of(n * COLS, COLS), COLS)
            back = dot(jac[0:rows, :], dec[:, at])
            h = hid[:, at]
            s = 1.0 - h * h
            sl = spread(second, s[0:1], s[1:2])
            up = back * sl
            lifted[0:rows, at] = up.astype(BF16)
            prod = back[EXTRA:] * along[EXTRA:rows, at]
            sec = second[EXTRA:]
            sum0 = jnp.sum(jnp.where(sec, 0.0, prod), axis=0, keepdims=True)
            sum1 = jnp.sum(jnp.where(sec, prod, 0.0), axis=0, keepdims=True)
            sc = -2.0 * h * s * spread(second[0:EXTRA], sum0, sum1)
            hi = sc.astype(BF16).astype(F32)
            mid = (sc - hi).astype(BF16).astype(F32)
            low = sc - hi - mid
            ent = up[0:EXTRA].astype(BF16).astype(F32)
            rest = jnp.where(extra_row < 6, mid, jnp.where(extra_row < 8, low, 0.0))
            fixed = jnp.where(extra_row < 2, ent, jnp.where(extra_row < 4, hi, rest))
            lifted[0:EXTRA, at] = fixed.astype(BF16)
            return carry

        lax.fori_loop(0, hidden // COLS, hidden_block, 0)
        transposed(cols, cols_t, in_width, depth)
        products(PER[1], cols_t, lifted, depth, in_width, hidden, table, both)

    by_size(EXTRA + r0 + r1, backward)
    encode_other(both, msg)


def own_terms(factor, ranks, table, x, y, dirs, targets, enc, dec):
    rmax = dirs.shape[1]
    in_width, hidden = enc.shape
    out_width = dec.shape[0]
    top, depth = SIZES[-1]
    blocks = 128
    shape = jax.ShapeDtypeStruct
    both, msg, jac, along, cols, hid, dec_v = pl.pallas_call(
        functools.partial(decoder_kernel, factor),
        out_shape=[
            shape((2 * blocks * PER[0], COLS), F32),
            shape((message_rows(((0, blocks),)), COLS), S16),
            shape((ROWS, out_width), BF16),
            shape((top, hidden), F32),
            shape((ROWS, in_width), BF16),
            shape((EXTRA, hidden), F32),
            shape(dec.shape, BF16),
        ],
        in_specs=[SM, SM, VM, VM, HB, HB, HB, HB],
        out_specs=[VM] * 7,
        scratch_shapes=[
            pltpu.VMEM(enc.shape, BF16),
            pltpu.VMEM(dirs.shape, BF16),
            pltpu.VMEM(targets.shape, BF16),
            pltpu.VMEM((ROWS, out_width), BF16),
            pltpu.VMEM((ROWS, hidden), BF16),
            pltpu.VMEM((out_width, depth), BF16),
            pltpu.SemaphoreType.DMA((4,)),
        ],
        compiler_params=pltpu.CompilerParams(vmem_limit_bytes=18 * MIB),
        cost_estimate=pl.CostEstimate(flops=int(8e9), transcendentals=0, bytes_accessed=0),
        name="decoder_terms",
    )(ranks, table, x, y, *[pltpu.with_memory_space_constraint(a, pltpu.HBM) for a in (dirs, targets, enc, dec)])
    both_e, msg_e = pl.pallas_call(
        encoder_kernel,
        out_shape=[
            shape((2 * blocks * PER[1], COLS), F32),
            shape((message_rows(((1, blocks),)), COLS), S16),
        ],
        in_specs=[SM, SM] + [VM] * 5,
        out_specs=[VM] * 2,
        scratch_shapes=[
            pltpu.VMEM((ROWS, hidden), BF16),
            pltpu.VMEM((in_width, depth), BF16),
        ],
        compiler_params=pltpu.CompilerParams(vmem_limit_bytes=10 * MIB),
        cost_estimate=pl.CostEstimate(flops=int(6e9), transcendentals=0, bytes_accessed=0),
        name="encoder_terms",
    )(ranks, table, jac, along, cols, hid, dec_v)
    return both, msg, both_e, msg_e


def z_partner(shift):
    return lambda z: (z + shift) % 8 if z % 2 == 0 else (z - shift) % 8


Z_SHIFTS = (1, -1, 3)


def z_place(z, zb):
    place = jnp.zeros_like(zb)
    for code in range(8):
        at, odd = z, z & 1
        for bit, shift in zip((4, 2, 1), Z_SHIFTS):
            if code & bit:
                at, odd = (at + jnp.where(odd == 0, shift, -shift)) & 7, 1 - odd
        place = place + jnp.where(at == zb, code, 0)
    return place


def place_table(z, y, core, x):
    i = jnp.arange(256, dtype=jnp.int32)
    xb, zb, yb, cb = i // 64, (i // 8) % 8, (i // 2) % 4, i % 2
    zp = z_place(z, zb)
    odd, zi = zp // 4, zp % 4
    first = cb == 0
    ea = jnp.where(first, xb ^ x, yb ^ y)
    eb = jnp.where(first, yb - y, xb - x) & 3
    ap = jnp.where(ea == 0, 0, jnp.where(ea == 2, 3, jnp.where((ea == 3) == (odd == 0), 1, 2)))
    group = jnp.where(cb == core, 0, 128)
    return group + odd * 64 + ap * 16 + eb * 4 + zi


def send(value, fn):
    pairs = []
    for z in range(8):
        for y in range(4):
            for c in range(2):
                for x in range(4):
                    z2, y2, c2, x2 = fn(z, y, c, x)
                    pairs.append((((z * 4 + y) * 2 + c) * 4 + x, ((z2 * 4 + y2) * 2 + c2) * 4 + x2))
    return lax.ppermute(value, ("dp", "mp"), pairs)


def other_core(z, y, c, x):
    return (z, y, 1 - c, x)


def first_axis(flip):
    return lambda z, y, c, x: (z, y, c, x ^ flip) if c == 0 else (z, y ^ flip, c, x)


def second_axis(k):
    return lambda z, y, c, x: (z, (y + k) % 4, c, x) if c == 0 else (z, y, c, (x + k) % 4)


def z_axis(shift):
    partner = z_partner(shift)
    return lambda z, y, c, x: (partner(z), y, c, x)


def per_device(sample_inputs, sample_outputs, directions, targets, ranks, enc, dec):
    population = sample_inputs.shape[0] * lax.axis_size("dp") * lax.axis_size("mp")
    factor = 2.0 / math.sqrt(population)
    dp = lax.axis_index("dp")
    x = lax.axis_index("mp")
    z, y, core = dp // 8, (dp // 2) % 4, dp % 2
    table = place_table(z, y, core, x)
    both_d, msg_d, both_e, msg_e = own_terms(
        factor, ranks, table, sample_inputs, sample_outputs, directions, targets, enc, dec
    )
    states, waiting = [], []
    for part, both, msg in ((0, both_d, msg_d), (1, both_e, msg_e)):
        tag = "de"[part]
        arrived = [send(msg, other_core)]
        state, msgs = reduce_step(
            "core_" + tag, (part,), core_groups(part), 64,
            (((part, 128),),), (((part, 32),),) * 2, (both,), arrived,
        )
        arrived = [send(m, first_axis(f)) for m, f in zip(msgs, (1, 3))]
        state, msgs = reduce_step(
            "first_" + tag, (part,), first_groups(part), 32,
            (((part, 32),),) * 2, (((part, 16),),) * 2, state, arrived,
        )
        states += state
        waiting += [send(m, first_axis(f)) for m, f in zip(msgs, (3, 1))]
    parts = (0, 1)
    states, msgs = reduce_step(
        "join", parts, join_groups(), 8,
        (((0, 16),),) * 2 + (((1, 16),),) * 2, (sections(8),) * 3, states, waiting,
    )
    arrived = [send(m, second_axis(k)) for m, k in zip(msgs, (1, 2, 3))]
    states, msgs = reduce_step(
        "second", parts, second_groups(), 4, (sections(8),) * 3, (sections(4),), states, arrived
    )
    arrived = [send(msgs[0], z_axis(Z_SHIFTS[0]))]
    states, msgs = reduce_step(
        "z_half", parts, half_groups(2), 2, (sections(4),), (sections(2),), states, arrived
    )
    arrived = [send(msgs[0], z_axis(Z_SHIFTS[1]))]
    states, msgs = reduce_step(
        "z_quarter", parts, half_groups(1), 1, (sections(2),), (sections(1),), states, arrived
    )
    arrived = [send(msgs[0], z_axis(Z_SHIFTS[2]))]
    states, _ = reduce_step(
        "z_last", parts, last_groups(), 1, (sections(1),), (), states, arrived
    )
    return states[1], states[0]


def solution(mesh):
    both = ("dp", "mp")
    in_specs = (
        P(both, None),
        P(both, None),
        P(both, None, None),
        P(both, None, None),
        P(both),
        P(),
        P(),
    )
    return jax.shard_map(
        per_device,
        mesh=mesh,
        in_specs=in_specs,
        out_specs=(P("dp", "mp"), P("dp", "mp")),
        check_vma=False,
    )
```

```python
import functools
import math

import jax
import jax.numpy as jnp
from jax import lax
from jax.experimental import pallas as pl
from jax.experimental.pallas import tpu as pltpu
from jax.sharding import PartitionSpec as P


F32 = jnp.float32
BF16 = jnp.bfloat16
S16 = jnp.int16
BLK = 16
EXTRA = 16
COLS = 512
PER = (16, 8)
TOP = 32700.0
TINY = 1e-30
MIB = 1 << 20
SIZES = ((256, 256), (416, 512), (528, 640))
ROWS = 784
RANKS_AT = 512

NN = (((1,), (0,)), ((), ()))
NT = (((1,), (1,)), ((), ()))
VM = pl.BlockSpec(memory_space=pltpu.VMEM)
SM = pl.BlockSpec(memory_space=pltpu.SMEM)
HB = pl.BlockSpec(memory_space=pltpu.HBM)


def dot(a, b, dims=NN):
    return lax.dot_general(a, b, dims, preferred_element_type=F32)


def section_base(sections, index):
    return sum(PER[p] * n for p, n in sections[:index])


def message(sections):
    rows = -(-section_base(sections, len(sections)) // 16) * 16 + 16
    return jax.ShapeDtypeStruct((rows, COLS), S16)


def exponents(largest):
    return jnp.floor(jnp.log(jnp.maximum(largest, TINY)) * (1.0 / math.log(2.0))) + 1.0


def power(e):
    return jnp.exp(e * math.log(2.0))


def tall(v, rows):
    return jnp.concatenate([v] * (rows // 8), axis=0) if rows > 8 else v


def coded(x, mult):
    return jnp.round(x * tall(mult, x.shape[0])).astype(jnp.int32).astype(S16)


def plain(q, mult):
    return q.astype(jnp.int32).astype(F32) * tall(mult, q.shape[0])


def fold_max(best, x):
    for r in range(0, x.shape[0], 8):
        best = jnp.maximum(best, jnp.abs(x[r : r + 8]))
    return best


def write_scales(msg, best):
    es = [exponents(b) for b in best]
    last = jnp.concatenate([es[0], es[-1]], axis=0).astype(jnp.int32).astype(S16)
    msg[msg.shape[0] - 16 :, :] = last
    return [power(-e) * TOP for e in es]


def read_scales(msg):
    e = msg[msg.shape[0] - 16 :, :].astype(jnp.int32).astype(F32)
    s = power(e) * (1.0 / TOP)
    return s[0:8], s[8:16]


def rows_loop(count, step, body, init):
    n = count // step
    if n == 1:
        return body(0, init)
    unroll = 4 if n % 4 == 0 else (2 if n % 2 == 0 else 1)

    def it(i, carry):
        for u in range(unroll):
            carry = body(pl.multiple_of((i * unroll + u) * step, step), carry)
        return carry

    return lax.fori_loop(0, n // unroll, it, init)


def encode_rows(src, src_start, count, msg, msg_start, mult):
    def body(o, carry):
        msg[pl.ds(msg_start + o, 16), :] = coded(src[pl.ds(src_start + o, 16), :], mult)
        return carry

    rows_loop(count, 16, body, 0)


def step_kernel(state_parts, parts, groups, ins, outs, *refs):
    ns, np_ = len(state_parts), len(parts)
    states, msgs = refs[:ns], refs[ns : ns + len(ins)]
    rest = refs[ns + len(ins) :]
    news = dict(zip(parts, rest[:np_]))
    sent = rest[np_ : np_ + len(outs)]
    holds = dict(zip(parts, rest[np_ + len(outs) :]))
    scales = [read_scales(m) for m in msgs]
    best = [[jnp.zeros((8, COLS), F32)] * len(o) for o in outs]
    pending = []
    held = {p: 0 for p in parts}
    for index, start, blocks, arrived, dest in groups:
        part = state_parts[index]
        per = PER[part]
        count = per * blocks
        step = min(16, count)

        def value(o, index=index, part=part, per=per, start=start, arrived=arrived, step=step):
            x = states[index][pl.ds(start * per + o, step), :]
            for m, at in arrived:
                where = [p for p, _ in ins[m]].index(part)
                base = section_base(ins[m], where) + per * at
                x = x + plain(msgs[m][pl.ds(base + o, step), :], scales[m][where])
            return x

        if dest[0] == "keep":

            def body(o, carry, value=value, part=part, to=dest[1] * per, step=step):
                news[part][pl.ds(to + o, step), :] = value(o)
                return carry

            rows_loop(count, step, body, 0)
        else:
            where = [p for p, _ in outs[dest[1]]].index(part)

            def body(o, carry, value=value, part=part, to=held[part], step=step):
                x = value(o)
                holds[part][pl.ds(to + o, step), :] = x
                return fold_max(carry, x)

            best[dest[1]][where] = rows_loop(count, step, body, best[dest[1]][where])
            pending.append((part, held[part], count, dest[1], where, dest[2] * per))
            held[part] += count
    mults = [write_scales(m, b) for m, b in zip(sent, best)]
    for part, at, count, j, where, to in pending:
        base = section_base(outs[j], where) + to
        if count < 16:
            sent[j][base : base + 8, :] = coded(holds[part][at : at + 8, :], mults[j][where])
            sent[j][base + 8 : base + 16, :] = jnp.zeros((8, COLS), S16)
        else:
            encode_rows(holds[part], at, count, sent[j], base, mults[j][where])


def reduce_step(state_parts, groups, keeps, ins, outs, states, msgs):
    parts = tuple(keeps)
    scratch = []
    if outs:
        for p in parts:
            held = sum(g[2] for g in groups if state_parts[g[0]] == p and g[4][0] == "send")
            scratch.append(pltpu.VMEM((held * PER[p], COLS), F32))
    out_shape = [jax.ShapeDtypeStruct((n * PER[p], COLS), F32) for p, n in keeps.items()]
    out_shape += [message(o) for o in outs]
    step = pl.pallas_call(
        functools.partial(step_kernel, state_parts, parts, groups, ins, outs),
        out_shape=out_shape,
        in_specs=[VM] * (len(states) + len(msgs)),
        out_specs=[VM] * len(out_shape),
        scratch_shapes=scratch,
        compiler_params=pltpu.CompilerParams(vmem_limit_bytes=16 * MIB),
        cost_estimate=pl.CostEstimate(flops=int(1e9), transcendentals=0, bytes_accessed=0),
    )
    got = step(*states, *msgs)
    return got[: len(parts)], got[len(parts) :]


def halves(index, start, n, source, at, keep, message_index):
    return (
        (index, start, n, ((source, at),), ("keep", keep)),
        (index, start + n, n, ((source, at + n),), ("send", message_index, 0)),
    )


def sections(n):
    return ((0, n), (1, n))


def reduced(both_d, msg_d, both_e, msg_e):
    whole_d, whole_e = ((0, 128),), ((1, 128),)
    got_d = sends([msg_d], [other_core])
    got_e = sends([msg_e], [other_core])
    dec_a, msgs_a = reduce_step(
        (0,), halves(0, 0, 48, 0, 0, 0, 0), {0: 48},
        (whole_d,), (((0, 48),),), [both_d], got_d,
    )
    got_a = sends(msgs_a, [first_axis(1)])
    state_b, msgs_b = reduce_step(
        (0, 1), halves(0, 96, 16, 0, 96, 0, 0) + halves(1, 0, 64, 1, 0, 0, 0),
        {0: 16, 1: 64}, (whole_d, whole_e), (((0, 16), (1, 64)),), [both_d, both_e], got_d + got_e,
    )
    got_b = sends(msgs_b, [first_axis(3)])
    dec_a, msgs_a = reduce_step(
        (0,), halves(0, 0, 24, 0, 0, 0, 0), {0: 24},
        (((0, 48),),), (((0, 24),),), dec_a, got_a,
    )
    got_a = sends(msgs_a, [first_axis(3)])
    state_b, msgs_b = reduce_step(
        (0, 1), halves(0, 0, 8, 0, 0, 0, 0) + halves(1, 0, 32, 0, 0, 0, 0),
        {0: 8, 1: 32}, (((0, 16), (1, 64)),), (((0, 8), (1, 32)),), state_b, got_b,
    )
    got_b = sends(msgs_b, [first_axis(1)])
    groups = ()
    for b in range(4):
        for index, n, source, to in ((0, 6, 0, 0), (1, 2, 1, 6), (2, 8, 1, 0)):
            dest = ("keep", to) if b == 0 else ("send", b - 1, to)
            groups += ((index, b * n, n, ((source, b * n),), dest),)
    both = (0, 1)
    states, msgs = reduce_step(
        (0, 0, 1), groups, {0: 8, 1: 8},
        (((0, 24),), ((0, 8), (1, 32))), (sections(8),) * 3, dec_a + state_b, got_a + got_b,
    )
    got = sends(msgs, [second_axis(k) for k in (1, 2, 3)])
    groups = ()
    for p in both:
        groups += ((p, 0, 4, tuple((k, 0) for k in range(3)), ("keep", 0)),)
        groups += ((p, 4, 4, tuple((k, 4) for k in range(3)), ("send", 0, 0)),)
    states, msgs = reduce_step(
        both, groups, {0: 4, 1: 4}, (sections(8),) * 3, (sections(4),), states, got
    )
    for i, n in ((0, 2), (1, 1)):
        got = sends(msgs, [z_axis(Z_SHIFTS[i])])
        states, msgs = reduce_step(
            both, halves(0, 0, n, 0, 0, 0, 0) + halves(1, 0, n, 0, 0, 0, 0),
            {0: n, 1: n}, (sections(2 * n),), (sections(n),), states, got,
        )
    got = sends(msgs, [z_axis(Z_SHIFTS[2])])
    groups = tuple((p, 0, 1, ((0, 0),), ("keep", 0)) for p in both)
    states, _ = reduce_step(both, groups, {0: 1, 1: 1}, (sections(1),), (), states, got)
    return states[1], states[0]


def by_size(total, body):
    low = 0
    for rows, depth in SIZES:

        @pl.when((total > low) & (total <= rows))
        def _(rows=rows, depth=depth):
            body(rows, depth)

        low = rows


def second_rows(rows, r0, width):
    row = lax.broadcasted_iota(jnp.int32, (rows, width), 0)
    return ((row < EXTRA) & (row % 2 == 1)) | (row >= EXTRA + r0)


def spread(second, v0, v1):
    return jnp.where(second, jnp.broadcast_to(v1, second.shape), jnp.broadcast_to(v0, second.shape))


def transposed(src, dst, width, depth):
    for k in range(0, depth, 128):
        for n in range(0, width, 512):
            dst[n : n + 512, k : k + 128] = src[k : k + 128, n : n + 512].T


def products(per, lhs_t, rhs, depth, width, hidden, table, base, both, best):
    def column_block(xb, carry):
        b = rhs[0:depth, pl.ds(pl.multiple_of(xb * COLS, COLS), COLS)]
        for n in range(0, width, 256):
            g = dot(lhs_t[n : n + 256, 0:depth], b)
            carry = fold_max(carry, g)
            for r in range(0, 256, per):
                to = table[base + xb * 64 + (n + r) // per]
                both[pl.ds(pl.multiple_of(to * per, per), per), :] = g[r : r + per]
        return carry

    best[...] = lax.fori_loop(0, hidden // COLS, column_block, jnp.zeros((8, COLS), F32))


def encode_other(both, best, msg):
    half = both.shape[0] // 2
    (mult,) = write_scales(msg, [best[...]])
    encode_rows(both, half, half, msg, 0, mult)


def decoder_kernel(
    factor, table, x_hbm, y_hbm, dirs, targets, enc, dec,
    both, msg, jac, along, cols, hid, dec_v,
    x_ref, y_ref, enc_v, dirs_v, targets_v, tgt, pushed, jac_t, best, sems,
):
    _, hidden = enc.shape
    out_width = dec.shape[0]
    rmax = dirs.shape[1]
    wide, high = hidden // 2, out_width // 2
    pairs = [(dirs, dirs_v), (x_hbm, x_ref)]
    pairs += [(enc.at[:, pl.ds(k, wide)], enc_v.at[:, pl.ds(k, wide)]) for k in (0, wide)]
    pairs += [(dec.at[pl.ds(0, high)], dec_v.at[pl.ds(0, high)]), (targets, targets_v)]
    pairs += [(y_hbm, y_ref), (dec.at[pl.ds(high, high)], dec_v.at[pl.ds(high, high)])]
    copies = [pltpu.make_async_copy(a, b, sems.at[i]) for i, (a, b) in enumerate(pairs)]
    for c in copies:
        c.start()
    r0, r1 = table[RANKS_AT], table[RANKS_AT + 1]
    at1 = pl.multiple_of(EXTRA + r0, BLK)
    tail = pl.multiple_of(EXTRA + rmax + r0, BLK)
    for ref in (cols, tgt):
        ref[pl.ds(tail, 256), :] = jnp.zeros((256, ref.shape[1]), BF16)

    def pair(ref):
        v = ref[...].astype(F32)
        odd = lax.broadcasted_iota(jnp.int32, (EXTRA, v.shape[1]), 0) % 2 == 1
        return spread(odd, v[0:1], v[1:2]).astype(BF16)

    copies[0].wait()
    cols[EXTRA : EXTRA + rmax, :] = dirs_v[0]
    cols[pl.ds(at1, rmax), :] = dirs_v[1]
    copies[1].wait()
    cols[0:EXTRA, :] = pair(x_ref)

    def forward(rows, depth):
        second = second_rows(rows, r0, COLS)
        first_row = lax.broadcasted_iota(jnp.int32, (rows, COLS), 0)
        if depth > rows:
            for ref in (pushed, jac):
                ref[rows:depth, :] = jnp.zeros((depth - rows, ref.shape[1]), BF16)

        for n in range(0, hidden, COLS):
            if n % wide == 0:
                copies[2 + n // wide].wait()
            at = slice(n, n + COLS)
            al = dot(cols[0:rows, :], enc_v[:, at])
            along[0:rows, at] = al
            h = jnp.tanh(al[0:EXTRA])
            hid[:, at] = h
            s = 1.0 - h * h
            sl = spread(second, s[0:1], s[1:2])
            pushed[0:rows, at] = (al * sl).astype(BF16)
            pushed[0:EXTRA, at] = h.astype(BF16)
        copies[5].wait()
        tgt[EXTRA : EXTRA + rmax, :] = targets_v[0]
        tgt[pl.ds(at1, rmax), :] = targets_v[1]
        copies[6].wait()
        tgt[0:EXTRA, :] = pair(y_ref)

        def weight_of(rank):
            return (factor * BLK) / jnp.full((rows, COLS), rank, jnp.int32).astype(F32)

        w = jnp.where(first_row >= EXTRA + r0, weight_of(r1), weight_of(r0))
        w = jnp.where(first_row < EXTRA, jnp.where(first_row < 2, factor, 0.0), w)
        w = jnp.where(first_row < EXTRA + r0 + r1, w, 0.0)

        for n in range(0, out_width, high):
            copies[4 if n == 0 else 7].wait()
            at = slice(n, n + high)
            im = dot(pushed[0:rows, :], dec_v[at, :], NT)
            jac[0:rows, at] = ((im - tgt[0:rows, at].astype(F32)) * w).astype(BF16)
        transposed(jac, jac_t, out_width, depth)
        products(PER[0], jac_t, pushed, depth, out_width, hidden, table, 0, both, best)

    by_size(EXTRA + r0 + r1, forward)
    encode_other(both, best, msg)


def encoder_kernel(
    table, jac, along, cols, hid, dec, both, msg, lifted, cols_t, best
):
    in_width = cols.shape[1]
    hidden = dec.shape[1]
    r0, r1 = table[RANKS_AT], table[RANKS_AT + 1]

    def backward(rows, depth):
        second = second_rows(rows, r0, COLS)
        extra_row = lax.broadcasted_iota(jnp.int32, (EXTRA, COLS), 0)
        if depth > rows:
            lifted[rows:depth, :] = jnp.zeros((depth - rows, hidden), BF16)

        def hidden_block(n, carry):
            at = pl.ds(pl.multiple_of(n * COLS, COLS), COLS)
            back = dot(jac[0:rows, :], dec[:, at])
            h = hid[:, at]
            s = 1.0 - h * h
            sl = spread(second, s[0:1], s[1:2])
            up = back * sl
            lifted[0:rows, at] = up.astype(BF16)
            prod = back[EXTRA:] * along[EXTRA:rows, at]
            sec = second[EXTRA:]
            sum0 = jnp.sum(jnp.where(sec, 0.0, prod), axis=0, keepdims=True)
            sum1 = jnp.sum(jnp.where(sec, prod, 0.0), axis=0, keepdims=True)
            sc = -2.0 * h * s * spread(second[0:EXTRA], sum0, sum1)
            hi = sc.astype(BF16).astype(F32)
            mid = (sc - hi).astype(BF16).astype(F32)
            low = sc - hi - mid
            ent = up[0:EXTRA].astype(BF16).astype(F32)
            rest = jnp.where(extra_row < 6, mid, jnp.where(extra_row < 8, low, 0.0))
            fixed = jnp.where(extra_row < 2, ent, jnp.where(extra_row < 4, hi, rest))
            lifted[0:EXTRA, at] = fixed.astype(BF16)
            return carry

        lax.fori_loop(0, hidden // COLS, hidden_block, 0)
        transposed(cols, cols_t, in_width, depth)
        products(PER[1], cols_t, lifted, depth, in_width, hidden, table, 256, both, best)

    by_size(EXTRA + r0 + r1, backward)
    encode_other(both, best, msg)


def own_terms(factor, table, x, y, dirs, targets, enc, dec):
    in_width, hidden = enc.shape
    out_width = dec.shape[0]
    top, depth = SIZES[-1]
    blocks = 128
    shape = jax.ShapeDtypeStruct
    both, msg, jac, along, cols, hid, dec_v = pl.pallas_call(
        functools.partial(decoder_kernel, factor),
        out_shape=[
            shape((2 * blocks * PER[0], COLS), F32),
            message(((0, blocks),)),
            shape((ROWS, out_width), BF16),
            shape((top, hidden), F32),
            shape((ROWS, in_width), BF16),
            shape((EXTRA, hidden), F32),
            shape(dec.shape, BF16),
        ],
        in_specs=[SM] + [HB] * 6,
        out_specs=[VM] * 7,
        scratch_shapes=[
            pltpu.VMEM(x.shape, BF16),
            pltpu.VMEM(y.shape, BF16),
            pltpu.VMEM(enc.shape, BF16),
            pltpu.VMEM(dirs.shape, BF16),
            pltpu.VMEM(targets.shape, BF16),
            pltpu.VMEM((ROWS, out_width), BF16),
            pltpu.VMEM((ROWS, hidden), BF16),
            pltpu.VMEM((out_width, depth), BF16),
            pltpu.VMEM((8, COLS), F32),
            pltpu.SemaphoreType.DMA((8,)),
        ],
        compiler_params=pltpu.CompilerParams(vmem_limit_bytes=18 * MIB),
        cost_estimate=pl.CostEstimate(flops=int(8e9), transcendentals=0, bytes_accessed=0),
        name="decoder_terms",
    )(table, *[pltpu.with_memory_space_constraint(a, pltpu.HBM) for a in (x, y, dirs, targets, enc, dec)])
    encoder_part = pl.pallas_call(
        encoder_kernel,
        out_shape=[
            shape((2 * blocks * PER[1], COLS), F32),
            message(((1, blocks),)),
        ],
        in_specs=[SM] + [VM] * 5,
        out_specs=[VM] * 2,
        scratch_shapes=[
            pltpu.VMEM((ROWS, hidden), BF16),
            pltpu.VMEM((in_width, depth), BF16),
            pltpu.VMEM((8, COLS), F32),
        ],
        compiler_params=pltpu.CompilerParams(vmem_limit_bytes=10 * MIB),
        cost_estimate=pl.CostEstimate(flops=int(6e9), transcendentals=0, bytes_accessed=0),
        name="encoder_terms",
    )
    both_e, msg_e = encoder_part(table, jac, along, cols, hid, dec_v)
    return both, msg, both_e, msg_e


Z_SHIFTS = (1, -1, 3)


def z_partner(shift, z, c):
    return (z + shift) % 8 if z % 2 == c else (z - shift) % 8


def z_place(z, zb, cb):
    place = jnp.zeros_like(zb)
    for code in range(8):
        at, odd = z, (z & 1) ^ cb
        for bit, shift in zip((4, 2, 1), Z_SHIFTS):
            if code & bit:
                at, odd = (at + jnp.where(odd == 0, shift, -shift)) & 7, 1 - odd
        place = place + jnp.where(at == zb, code, 0)
    return place


def place_table(z, y, core, x, ranks):
    i = jnp.arange(640, dtype=jnp.int32)
    xb, zb, yb, cb = (i >> 6) & 3, (i >> 3) & 7, (i >> 1) & 3, i & 1
    encoder = i >= 256
    zp = z_place(z, zb, cb)
    lane_b = encoder | (zp >= 6)
    first = cb == 0
    ea = jnp.where(first, xb ^ x, yb ^ y)
    eb = jnp.where(first, yb - y, xb - x) & 3
    ap = jnp.where(ea == 0, 0, jnp.where(ea == 2, 3, jnp.where((ea == 1) == lane_b, 1, 2)))
    rest = jnp.where(lane_b, 96 + ap * 8 + eb * 2 + zp - 6, ap * 24 + eb * 6 + zp)
    place = jnp.where(cb == core, 0, 128) + jnp.where(encoder, ap * 32 + eb * 8 + zp, rest)
    return jnp.where(i < RANKS_AT, place, 0) + jnp.pad(ranks, (RANKS_AT, 126))


def send(value, fn):
    pairs = []
    for z in range(8):
        for y in range(4):
            for c in range(2):
                for x in range(4):
                    z2, y2, c2, x2 = fn(z, y, c, x)
                    pairs.append((((z * 4 + y) * 2 + c) * 4 + x, ((z2 * 4 + y2) * 2 + c2) * 4 + x2))
    return lax.ppermute(value, ("dp", "mp"), pairs)


def sends(values, ways):
    got = []
    for v, way in zip(values, ways):
        got.append(send(v, way))
    return got


def other_core(z, y, c, x):
    return (z, y, 1 - c, x)


def first_axis(flip):
    return lambda z, y, c, x: (z, y, c, x ^ flip) if c == 0 else (z, y ^ flip, c, x)


def second_axis(k):
    return lambda z, y, c, x: (z, (y + k) % 4, c, x) if c == 0 else (z, y, c, (x + k) % 4)


def z_axis(shift):
    return lambda z, y, c, x: (z_partner(shift, z, c), y, c, x)


def per_device(sample_inputs, sample_outputs, directions, targets, ranks, enc, dec):
    population = sample_inputs.shape[0] * lax.axis_size("dp") * lax.axis_size("mp")
    factor = 2.0 / math.sqrt(population)
    dp = lax.axis_index("dp")
    x = lax.axis_index("mp")
    z, y, core = dp // 8, (dp // 2) % 4, dp % 2
    table = place_table(z, y, core, x, ranks)
    both_d, msg_d, both_e, msg_e = own_terms(
        factor, table, sample_inputs, sample_outputs, directions, targets, enc, dec
    )
    return reduced(both_d, msg_d, both_e, msg_e)


def solution(mesh):
    both = ("dp", "mp")
    in_specs = (
        P(both, None),
        P(both, None),
        P(both, None, None),
        P(both, None, None),
        P(both),
        P(),
        P(),
    )

    return jax.shard_map(
        per_device,
        mesh=mesh,
        in_specs=in_specs,
        out_specs=(P("dp", "mp"), P("dp", "mp")),
        check_vma=False,
    )
```

```python
import functools
import math

import jax
import jax.numpy as jnp
from jax import lax
from jax.experimental import pallas as pl
from jax.experimental.pallas import tpu as pltpu
from jax.sharding import PartitionSpec as P


F32 = jnp.float32
BF16 = jnp.bfloat16
S16 = jnp.int16
BLK = 16
EXTRA = 16
COLS = 512
PER = (16, 8)
TOP = 32700.0
TINY = 1e-30
MIB = 1 << 20
SIZES = ((256, 256), (416, 512), (528, 640))
ROWS = 784
RANKS_AT = 512

NN = (((1,), (0,)), ((), ()))
NT = (((1,), (1,)), ((), ()))
VM = pl.BlockSpec(memory_space=pltpu.VMEM)
SM = pl.BlockSpec(memory_space=pltpu.SMEM)
HB = pl.BlockSpec(memory_space=pltpu.HBM)


def dot(a, b, dims=NN):
    return lax.dot_general(a, b, dims, preferred_element_type=F32)


def section_base(sections, index):
    return sum(PER[p] * n for p, n in sections[:index])


def message(sections):
    rows = section_base(sections, len(sections)) + 8
    return jax.ShapeDtypeStruct((rows, COLS), S16)


def exponents(largest):
    return jnp.floor(jnp.log(jnp.maximum(largest, TINY)) * (1.0 / math.log(2.0))) + 1.0


def power(e):
    return jnp.exp(e * math.log(2.0))


def tall(v, rows):
    return jnp.concatenate([v] * (rows // 8), axis=0) if rows > 8 else v


def coded(x, mult):
    return jnp.round(x * tall(mult, x.shape[0])).astype(jnp.int32).astype(S16)


def plain(q, mult):
    return q.astype(jnp.int32).astype(F32) * tall(mult, q.shape[0])


def fold_max(best, x):
    for r in range(0, x.shape[0], 8):
        best = jnp.maximum(best, jnp.abs(x[r : r + 8]))
    return best


def quads(best):
    top = lax.broadcasted_iota(jnp.int32, (8, COLS), 0) < 4
    es = [exponents(jnp.maximum(b, pltpu.roll(b, 4, 0))) for b in best]
    return es, jnp.where(top, es[0], es[-1]).astype(jnp.int32).astype(S16)


def write_scales(msg, best):
    es, rows = quads(best)
    at = msg.shape[0] - 8
    if at % 16 == 0:
        msg[at:, :] = rows
    return [power(-e) * TOP for e in es], rows


def read_scales(msg):
    top = lax.broadcasted_iota(jnp.int32, (8, COLS), 0) < 4
    at = msg.shape[0] - 8
    tile = msg[at // 16 * 16 :, :].astype(jnp.int32).astype(F32)
    e = tile[tile.shape[0] - 8 :]
    other = pltpu.roll(e, 4, 0)
    scale = 1.0 / TOP
    return power(jnp.where(top, e, other)) * scale, power(jnp.where(top, other, e)) * scale


def rows_loop(count, step, body, init):
    n = count // step
    if n == 1:
        return body(0, init)
    unroll = 4 if n % 4 == 0 else (2 if n % 2 == 0 else 1)

    def it(i, carry):
        for u in range(unroll):
            carry = body(pl.multiple_of((i * unroll + u) * step, step), carry)
        return carry

    return lax.fori_loop(0, n // unroll, it, init)


def encode_rows(src, src_start, count, msg, msg_start, mult):
    def body(o, carry):
        msg[pl.ds(msg_start + o, 16), :] = coded(src[pl.ds(src_start + o, 16), :], mult)
        return carry

    rows_loop(count, 16, body, 0)


def step_kernel(state_parts, parts, groups, ins, outs, *refs):
    ns, np_ = len(state_parts), len(parts)
    states, msgs = refs[:ns], refs[ns : ns + len(ins)]
    rest = refs[ns + len(ins) :]
    news = dict(zip(parts, rest[:np_]))
    sent = rest[np_ : np_ + len(outs)]
    holds = dict(zip(parts, rest[np_ + len(outs) :]))
    scales = [read_scales(m) for m in msgs]
    best = [[jnp.zeros((8, COLS), F32)] * len(o) for o in outs]
    pending = []
    held = {p: 0 for p in parts}
    for index, start, blocks, arrived, dest in groups:
        part = state_parts[index]
        per = PER[part]
        count = per * blocks
        step = min(16, count)

        def value(o, index=index, part=part, per=per, start=start, arrived=arrived, step=step):
            x = states[index][pl.ds(start * per + o, step), :]
            for m, at in arrived:
                where = [p for p, _ in ins[m]].index(part)
                base = section_base(ins[m], where) + per * at
                x = x + plain(msgs[m][pl.ds(base + o, step), :], scales[m][where])
            return x

        if dest[0] == "keep":

            def body(o, carry, value=value, part=part, to=dest[1] * per, step=step):
                news[part][pl.ds(to + o, step), :] = value(o)
                return carry

            rows_loop(count, step, body, 0)
        else:
            where = [p for p, _ in outs[dest[1]]].index(part)

            def body(o, carry, value=value, part=part, to=held[part], step=step):
                x = value(o)
                holds[part][pl.ds(to + o, step), :] = x
                return fold_max(carry, x)

            best[dest[1]][where] = rows_loop(count, step, body, best[dest[1]][where])
            pending.append((part, held[part], count, dest[1], where, dest[2] * per))
            held[part] += count
    coding = [write_scales(m, b) for m, b in zip(sent, best)]
    for part, at, count, j, where, to in pending:
        base = section_base(outs[j], where) + to
        if count < 16:
            last = coded(holds[part][at : at + 8, :], coding[j][0][where])
            sent[j][base : base + 16, :] = jnp.concatenate([last, coding[j][1]], axis=0)
        else:
            encode_rows(holds[part], at, count, sent[j], base, coding[j][0][where])


def reduce_step(state_parts, groups, keeps, ins, outs, states, msgs):
    parts = tuple(keeps)
    scratch = []
    if outs:
        for p in parts:
            held = sum(g[2] for g in groups if state_parts[g[0]] == p and g[4][0] == "send")
            scratch.append(pltpu.VMEM((held * PER[p], COLS), F32))
    out_shape = [jax.ShapeDtypeStruct((n * PER[p], COLS), F32) for p, n in keeps.items()]
    out_shape += [message(o) for o in outs]
    step = pl.pallas_call(
        functools.partial(step_kernel, state_parts, parts, groups, ins, outs),
        out_shape=out_shape,
        in_specs=[VM] * (len(states) + len(msgs)),
        out_specs=[VM] * len(out_shape),
        scratch_shapes=scratch,
        compiler_params=pltpu.CompilerParams(vmem_limit_bytes=16 * MIB),
        cost_estimate=pl.CostEstimate(flops=int(1e9), transcendentals=0, bytes_accessed=0),
    )
    got = step(*states, *msgs)
    return got[: len(parts)], got[len(parts) :]


def halves(index, start, n, source, at, keep, message_index):
    return (
        (index, start, n, ((source, at),), ("keep", keep)),
        (index, start + n, n, ((source, at + n),), ("send", message_index, 0)),
    )


def sections(n):
    return ((0, n), (1, n))


def reduced(both_d, msg_d, both_e, msg_e):
    whole_d, whole_e = ((0, 128),), ((1, 128),)
    got_d = sends([msg_d], [other_core])
    got_e = sends([msg_e], [other_core])
    dec_a, msgs_a = reduce_step(
        (0,), halves(0, 0, 56, 0, 0, 0, 0), {0: 56},
        (whole_d,), (((0, 56),),), [both_d], got_d,
    )
    got_a = sends(msgs_a, [first_axis(1)])
    state_b, msgs_b = reduce_step(
        (0, 1), halves(0, 112, 8, 0, 112, 0, 0) + halves(1, 0, 64, 1, 0, 0, 0),
        {0: 8, 1: 64}, (whole_d, whole_e), (((0, 8), (1, 64)),), [both_d, both_e], got_d + got_e,
    )
    got_b = sends(msgs_b, [first_axis(3)])
    dec_a, msgs_a = reduce_step(
        (0,), halves(0, 0, 28, 0, 0, 0, 0), {0: 28},
        (((0, 56),),), (((0, 28),),), dec_a, got_a,
    )
    got_a = sends(msgs_a, [first_axis(3)])
    state_b, msgs_b = reduce_step(
        (0, 1), halves(0, 0, 4, 0, 0, 0, 0) + halves(1, 0, 32, 0, 0, 0, 0),
        {0: 4, 1: 32}, (((0, 8), (1, 64)),), (((0, 4), (1, 32)),), state_b, got_b,
    )
    got_b = sends(msgs_b, [first_axis(1)])
    groups = ()
    for b in range(4):
        for index, n, source, to in ((0, 7, 0, 0), (1, 1, 1, 7), (2, 8, 1, 0)):
            dest = ("keep", to) if b == 0 else ("send", b - 1, to)
            groups += ((index, b * n, n, ((source, b * n),), dest),)
    both = (0, 1)
    states, msgs = reduce_step(
        (0, 0, 1), groups, {0: 8, 1: 8},
        (((0, 28),), ((0, 4), (1, 32))), (sections(8),) * 3, dec_a + state_b, got_a + got_b,
    )
    got = sends(msgs, [second_axis(k) for k in (1, 2, 3)])
    groups = ()
    for p in both:
        groups += ((p, 0, 4, tuple((k, 0) for k in range(3)), ("keep", 0)),)
        groups += ((p, 4, 4, tuple((k, 4) for k in range(3)), ("send", 0, 0)),)
    states, msgs = reduce_step(
        both, groups, {0: 4, 1: 4}, (sections(8),) * 3, (sections(4),), states, got
    )
    for i, n in ((0, 2), (1, 1)):
        got = sends(msgs, [z_axis(Z_SHIFTS[i])])
        states, msgs = reduce_step(
            both, halves(0, 0, n, 0, 0, 0, 0) + halves(1, 0, n, 0, 0, 0, 0),
            {0: n, 1: n}, (sections(2 * n),), (sections(n),), states, got,
        )
    got = sends(msgs, [z_axis(Z_SHIFTS[2])])
    groups = tuple((p, 0, 1, ((0, 0),), ("keep", 0)) for p in both)
    states, _ = reduce_step(both, groups, {0: 1, 1: 1}, (sections(1),), (), states, got)
    return states[1], states[0]


def by_size(total, body):
    low = 0
    for rows, depth in SIZES:

        @pl.when((total > low) & (total <= rows))
        def _(rows=rows, depth=depth):
            body(rows, depth)

        low = rows


def second_rows(rows, r0, width):
    row = lax.broadcasted_iota(jnp.int32, (rows, width), 0)
    return ((row < EXTRA) & (row % 2 == 1)) | (row >= EXTRA + r0)


def spread(second, v0, v1):
    return jnp.where(second, jnp.broadcast_to(v1, second.shape), jnp.broadcast_to(v0, second.shape))


def transposed(src, dst, width, depth):
    for k in range(0, depth, 128):
        for n in range(0, width, 512):
            dst[n : n + 512, k : k + 128] = src[k : k + 128, n : n + 512].T


def products(per, lhs_t, rhs, depth, width, hidden, table, base, both, best):
    def column_block(xb, carry):
        b = rhs[0:depth, pl.ds(pl.multiple_of(xb * COLS, COLS), COLS)]
        for n in range(0, width, 256):
            g = dot(lhs_t[n : n + 256, 0:depth], b)
            carry = fold_max(carry, g)
            for r in range(0, 256, per):
                to = table[base + xb * 64 + (n + r) // per]
                both[pl.ds(pl.multiple_of(to * per, per), per), :] = g[r : r + per]
        return carry

    best[...] = lax.fori_loop(0, hidden // COLS, column_block, jnp.zeros((8, COLS), F32))


def encode_other(both, best, msg):
    half = both.shape[0] // 2
    ((mult,), _) = write_scales(msg, [best[...]])
    encode_rows(both, half, half, msg, 0, mult)


def decoder_kernel(
    factor, table, x_hbm, y_hbm, dirs, targets, enc, dec,
    both, msg, jac, along, cols, hid, dec_v,
    x_ref, y_ref, enc_v, dirs_v, targets_v, tgt, pushed, jac_t, best, sems,
):
    _, hidden = enc.shape
    out_width = dec.shape[0]
    rmax = dirs.shape[1]
    wide, high = hidden // 2, out_width // 2
    pairs = [(dirs, dirs_v), (x_hbm, x_ref)]
    pairs += [(enc.at[:, pl.ds(k, wide)], enc_v.at[:, pl.ds(k, wide)]) for k in (0, wide)]
    pairs += [(dec.at[pl.ds(0, high)], dec_v.at[pl.ds(0, high)]), (targets, targets_v)]
    pairs += [(y_hbm, y_ref), (dec.at[pl.ds(high, high)], dec_v.at[pl.ds(high, high)])]
    copies = [pltpu.make_async_copy(a, b, sems.at[i]) for i, (a, b) in enumerate(pairs)]
    for c in copies:
        c.start()
    r0, r1 = table[RANKS_AT], table[RANKS_AT + 1]
    at1 = pl.multiple_of(EXTRA + r0, BLK)
    tail = pl.multiple_of(EXTRA + rmax + r0, BLK)
    for ref in (cols, tgt):
        ref[pl.ds(tail, 256), :] = jnp.zeros((256, ref.shape[1]), BF16)

    def pair(ref):
        v = ref[...].astype(F32)
        odd = lax.broadcasted_iota(jnp.int32, (EXTRA, v.shape[1]), 0) % 2 == 1
        return spread(odd, v[0:1], v[1:2]).astype(BF16)

    copies[0].wait()
    cols[EXTRA : EXTRA + rmax, :] = dirs_v[0]
    cols[pl.ds(at1, rmax), :] = dirs_v[1]
    copies[1].wait()
    cols[0:EXTRA, :] = pair(x_ref)

    def forward(rows, depth):
        second = second_rows(rows, r0, COLS)
        first_row = lax.broadcasted_iota(jnp.int32, (rows, COLS), 0)
        if depth > rows:
            for ref in (pushed, jac):
                ref[rows:depth, :] = jnp.zeros((depth - rows, ref.shape[1]), BF16)

        for n in range(0, hidden, COLS):
            if n % wide == 0:
                copies[2 + n // wide].wait()
            at = slice(n, n + COLS)
            al = dot(cols[0:rows, :], enc_v[:, at])
            along[0:rows, at] = al
            h = jnp.tanh(al[0:EXTRA])
            hid[:, at] = h
            s = 1.0 - h * h
            sl = spread(second, s[0:1], s[1:2])
            pushed[0:rows, at] = (al * sl).astype(BF16)
            pushed[0:EXTRA, at] = h.astype(BF16)
        copies[5].wait()
        tgt[EXTRA : EXTRA + rmax, :] = targets_v[0]
        tgt[pl.ds(at1, rmax), :] = targets_v[1]
        copies[6].wait()
        tgt[0:EXTRA, :] = pair(y_ref)

        def weight_of(rank):
            return (factor * BLK) / jnp.full((rows, COLS), rank, jnp.int32).astype(F32)

        w = jnp.where(first_row >= EXTRA + r0, weight_of(r1), weight_of(r0))
        w = jnp.where(first_row < EXTRA, jnp.where(first_row < 2, factor, 0.0), w)
        w = jnp.where(first_row < EXTRA + r0 + r1, w, 0.0)

        for n in range(0, out_width, high):
            copies[4 if n == 0 else 7].wait()
            at = slice(n, n + high)
            im = dot(pushed[0:rows, :], dec_v[at, :], NT)
            jac[0:rows, at] = ((im - tgt[0:rows, at].astype(F32)) * w).astype(BF16)
        transposed(jac, jac_t, out_width, depth)
        products(PER[0], jac_t, pushed, depth, out_width, hidden, table, 0, both, best)

    by_size(EXTRA + r0 + r1, forward)
    encode_other(both, best, msg)


def encoder_kernel(
    table, jac, along, cols, hid, dec, both, msg, lifted, cols_t, best
):
    in_width = cols.shape[1]
    hidden = dec.shape[1]
    r0, r1 = table[RANKS_AT], table[RANKS_AT + 1]

    def backward(rows, depth):
        second = second_rows(rows, r0, COLS)
        extra_row = lax.broadcasted_iota(jnp.int32, (EXTRA, COLS), 0)
        if depth > rows:
            lifted[rows:depth, :] = jnp.zeros((depth - rows, hidden), BF16)

        def hidden_block(n, carry):
            at = pl.ds(pl.multiple_of(n * COLS, COLS), COLS)
            back = dot(jac[0:rows, :], dec[:, at])
            h = hid[:, at]
            s = 1.0 - h * h
            sl = spread(second, s[0:1], s[1:2])
            up = back * sl
            lifted[0:rows, at] = up.astype(BF16)
            prod = back[EXTRA:] * along[EXTRA:rows, at]
            sec = second[EXTRA:]
            sum0 = jnp.sum(jnp.where(sec, 0.0, prod), axis=0, keepdims=True)
            sum1 = jnp.sum(jnp.where(sec, prod, 0.0), axis=0, keepdims=True)
            sc = -2.0 * h * s * spread(second[0:EXTRA], sum0, sum1)
            hi = sc.astype(BF16).astype(F32)
            mid = (sc - hi).astype(BF16).astype(F32)
            low = sc - hi - mid
            ent = up[0:EXTRA].astype(BF16).astype(F32)
            rest = jnp.where(extra_row < 6, mid, jnp.where(extra_row < 8, low, 0.0))
            fixed = jnp.where(extra_row < 2, ent, jnp.where(extra_row < 4, hi, rest))
            lifted[0:EXTRA, at] = fixed.astype(BF16)
            return carry

        lax.fori_loop(0, hidden // COLS, hidden_block, 0)
        transposed(cols, cols_t, in_width, depth)
        products(PER[1], cols_t, lifted, depth, in_width, hidden, table, 256, both, best)

    by_size(EXTRA + r0 + r1, backward)
    encode_other(both, best, msg)


def own_terms(factor, table, x, y, dirs, targets, enc, dec):
    in_width, hidden = enc.shape
    out_width = dec.shape[0]
    top, depth = SIZES[-1]
    blocks = 128
    shape = jax.ShapeDtypeStruct
    both, msg, jac, along, cols, hid, dec_v = pl.pallas_call(
        functools.partial(decoder_kernel, factor),
        out_shape=[
            shape((2 * blocks * PER[0], COLS), F32),
            message(((0, blocks),)),
            shape((ROWS, out_width), BF16),
            shape((top, hidden), F32),
            shape((ROWS, in_width), BF16),
            shape((EXTRA, hidden), F32),
            shape(dec.shape, BF16),
        ],
        in_specs=[SM] + [HB] * 6,
        out_specs=[VM] * 7,
        scratch_shapes=[
            pltpu.VMEM(x.shape, BF16),
            pltpu.VMEM(y.shape, BF16),
            pltpu.VMEM(enc.shape, BF16),
            pltpu.VMEM(dirs.shape, BF16),
            pltpu.VMEM(targets.shape, BF16),
            pltpu.VMEM((ROWS, out_width), BF16),
            pltpu.VMEM((ROWS, hidden), BF16),
            pltpu.VMEM((out_width, depth), BF16),
            pltpu.VMEM((8, COLS), F32),
            pltpu.SemaphoreType.DMA((8,)),
        ],
        compiler_params=pltpu.CompilerParams(vmem_limit_bytes=18 * MIB),
        cost_estimate=pl.CostEstimate(flops=int(8e9), transcendentals=0, bytes_accessed=0),
        name="decoder_terms",
    )(table, *[pltpu.with_memory_space_constraint(a, pltpu.HBM) for a in (x, y, dirs, targets, enc, dec)])
    encoder_part = pl.pallas_call(
        encoder_kernel,
        out_shape=[
            shape((2 * blocks * PER[1], COLS), F32),
            message(((1, blocks),)),
        ],
        in_specs=[SM] + [VM] * 5,
        out_specs=[VM] * 2,
        scratch_shapes=[
            pltpu.VMEM((ROWS, hidden), BF16),
            pltpu.VMEM((in_width, depth), BF16),
            pltpu.VMEM((8, COLS), F32),
        ],
        compiler_params=pltpu.CompilerParams(vmem_limit_bytes=10 * MIB),
        cost_estimate=pl.CostEstimate(flops=int(6e9), transcendentals=0, bytes_accessed=0),
        name="encoder_terms",
    )
    both_e, msg_e = encoder_part(table, jac, along, cols, hid, dec_v)
    return both, msg, both_e, msg_e


Z_SHIFTS = (1, -1, 3)


def z_partner(shift, z, c):
    return (z + shift) % 8 if z % 2 == c else (z - shift) % 8


def z_place(z, zb, cb):
    place = jnp.zeros_like(zb)
    for code in range(8):
        at, odd = z, (z & 1) ^ cb
        for bit, shift in zip((4, 2, 1), Z_SHIFTS):
            if code & bit:
                at, odd = (at + jnp.where(odd == 0, shift, -shift)) & 7, 1 - odd
        place = place + jnp.where(at == zb, code, 0)
    return place


def place_table(z, y, core, x, ranks):
    i = jnp.arange(640, dtype=jnp.int32)
    xb, zb, yb, cb = (i >> 6) & 3, (i >> 3) & 7, (i >> 1) & 3, i & 1
    encoder = i >= 256
    zp = z_place(z, zb, cb)
    lane_b = encoder | (zp >= 7)
    first = cb == 0
    ea = jnp.where(first, xb ^ x, yb ^ y)
    eb = jnp.where(first, yb - y, xb - x) & 3
    ap = jnp.where(ea == 0, 0, jnp.where(ea == 2, 3, jnp.where((ea == 1) == lane_b, 1, 2)))
    rest = jnp.where(lane_b, 112 + ap * 4 + eb, ap * 28 + eb * 7 + zp)
    place = jnp.where(cb == core, 0, 128) + jnp.where(encoder, ap * 32 + eb * 8 + zp, rest)
    return jnp.where(i < RANKS_AT, place, 0) + jnp.pad(ranks, (RANKS_AT, 126))


def send(value, fn):
    pairs = []
    for z in range(8):
        for y in range(4):
            for c in range(2):
                for x in range(4):
                    z2, y2, c2, x2 = fn(z, y, c, x)
                    pairs.append((((z * 4 + y) * 2 + c) * 4 + x, ((z2 * 4 + y2) * 2 + c2) * 4 + x2))
    return lax.ppermute(value, ("dp", "mp"), pairs)


def sends(values, ways):
    got = []
    for v, way in zip(values, ways):
        got.append(send(v, way))
    return got


def other_core(z, y, c, x):
    return (z, y, 1 - c, x)


def first_axis(flip):
    return lambda z, y, c, x: (z, y, c, x ^ flip) if c == 0 else (z, y ^ flip, c, x)


def second_axis(k):
    return lambda z, y, c, x: (z, (y + k) % 4, c, x) if c == 0 else (z, y, c, (x + k) % 4)


def z_axis(shift):
    return lambda z, y, c, x: (z_partner(shift, z, c), y, c, x)


def per_device(sample_inputs, sample_outputs, directions, targets, ranks, enc, dec):
    population = sample_inputs.shape[0] * lax.axis_size("dp") * lax.axis_size("mp")
    factor = 2.0 / math.sqrt(population)
    dp = lax.axis_index("dp")
    x = lax.axis_index("mp")
    z, y, core = dp // 8, (dp // 2) % 4, dp % 2
    table = place_table(z, y, core, x, ranks)
    both_d, msg_d, both_e, msg_e = own_terms(
        factor, table, sample_inputs, sample_outputs, directions, targets, enc, dec
    )
    return reduced(both_d, msg_d, both_e, msg_e)


def solution(mesh):
    both = ("dp", "mp")
    in_specs = (
        P(both, None),
        P(both, None),
        P(both, None, None),
        P(both, None, None),
        P(both),
        P(),
        P(),
    )

    return jax.shard_map(
        per_device,
        mesh=mesh,
        in_specs=in_specs,
        out_specs=(P("dp", "mp"), P("dp", "mp")),
        check_vma=False,
    )
```
